32 devices in a mesh: bead: 8 (over z, core), atom: 4 (over y, x).
Axes of the slice: x: 2, y: 2, z: 4, core: 2. Of those that a mesh axis runs over, the one named last changes fastest.
Arguments:
- positions: float32 [32, 3, 4096], P('bead', None, 'atom'), may hold values from -6 to 6
- momenta: float32 [32, 3, 4096], P('bead', None, 'atom'), may hold values from -6 to 6
- charge: float32 [4096], P('atom'), may hold values from -1 to 1
- masses: float32 [4096], P('atom'), may hold values from 0.5 to 4
- pair_local: int32 [128], P('atom'), may hold values from 0 to 31, as said below
- pair_other: int32 [128], P('atom'), may hold values from 0 to 31, as said below
- pair_count: int32 [4], P('atom'), may hold values from 0 to 32, as said below
Outputs:
- new_positions: float32 [32, 3, 4096], P('bead', None, 'atom')
- new_momenta: float32 [32, 3, 4096], P('bead', None, 'atom')
- spring: float32 [4096], P('atom')
The draws below stay inside these ranges and needn't reach their ends.
Inputs may be any that keep to these rules, and one draw needn't show every extreme that they name: `pair_local`: the slots of atom block d (slots d * 32 to (d + 1) * 32 - 1) name tiles of that block: d * 8 to (d + 1) * 8 - 1. `pair_other`: each slot's neighbour tile lies within 8 tiles of its tile, counting cyclically over 32 tiles. `pair_count`: the counts of blocks d and d + 2 sum to at most 32.
All inputs are finite; a program needn't handle non-finite values.
Results may differ from the reference program's by a relative error of at most 0.000071.
Values sent between devices are 32-bit elements; how exact they have to be, the bound alone decides.
A program may use at most 64 MiB of HBM per device.

```python
import math
import jax
import jax.numpy as jnp
from jax import lax

TILE_ATOMS = 128
TILE_DEV = 8
PAIR_DEV = 32
BEADS = 32
ATOMS = 4096
TILES = 32
PAIRS = 128
N_ATOM = 4


def pair_plan(key):
    base_key = jax.random.fold_in(key, 7)
    keys = jax.random.split(base_key, 6)
    halves = N_ATOM // 2
    heavy = jax.random.randint(keys[0], (halves,), PAIR_DEV // 2 + 1, PAIR_DEV + 1)
    chosen = jax.random.randint(keys[1], (), 0, halves)
    heavy = jnp.where(jnp.arange(halves) == chosen, PAIR_DEV, heavy)
    light = jax.random.randint(keys[2], (halves,), 0, PAIR_DEV - heavy + 1)
    sides = jax.random.randint(keys[3], (halves,), 0, 2)
    lower = jnp.where(sides == 1, heavy, light)
    upper = jnp.where(sides == 1, light, heavy)
    counts = jnp.concatenate([lower, upper]).astype(jnp.int32)
    local = jax.random.randint(keys[4], (N_ATOM, PAIR_DEV), 0, TILE_DEV) + jnp.arange(N_ATOM)[:, None] * TILE_DEV
    offsets = jax.random.randint(keys[5], (N_ATOM, PAIR_DEV), -TILE_DEV, TILE_DEV + 1)
    other = (local + offsets) % (TILE_DEV * N_ATOM)
    return (counts, local.reshape(-1).astype(jnp.int32), other.reshape(-1).astype(jnp.int32))


def draw_pair_local(key, part):
    return pair_plan(key)[1]


def draw_pair_other(key, part):
    return pair_plan(key)[2]


def draw_pair_count(key, part):
    return pair_plan(key)[0]


def block_scale(own_key, shape, pieces, low, largest):
    loudness = 1.0
    for dim, shards_of in pieces:
        heights = jax.random.uniform(jax.random.fold_in(jax.random.fold_in(own_key, 6), dim), (shards_of,), jnp.float32, low / len(pieces), largest / len(pieces))
        loudness = loudness * jnp.repeat(jnp.exp(heights), shape[dim] // shards_of).reshape((-1,) + (1,) * (len(shape) - 1 - dim))
    return loudness


def noise(rng, dims, spread, most, pieces=(), held_as=jnp.bfloat16):
    drawn = jax.random.normal(rng, dims, jnp.float32) * spread
    if len(pieces) > 0:
        drawn = block_scale(rng, dims, pieces, -0.22, 0.18) * drawn
    return jnp.clip(drawn, min=-most, max=most).astype(held_as)


def setup_inputs(seed: int = 0) -> dict:
    key_of = jax.random.split(jax.random.key(seed), 8)
    return {
        "positions": noise(key_of[0], (BEADS, 3, ATOMS), 1.0, 6.0, ((0, 8), (2, 4)), jnp.float32),
        "momenta": noise(key_of[1], (BEADS, 3, ATOMS), 1.0, 6.0, ((0, 8), (2, 4)), jnp.float32),
        "charge": jnp.clip(jax.random.uniform(key_of[2], (ATOMS,), jnp.float32, -1.0, 1.0) * block_scale(key_of[2], (ATOMS,), ((0, 4),), -0.4, 0.0), -1.0, 1.0),
        "masses": jnp.clip(jnp.exp(math.log(4.0) - 2.0794415 * jax.random.uniform(key_of[3], (ATOMS,), jnp.float32) ** block_scale(key_of[3], (ATOMS,), ((0, 4),), -0.2, 0.2)), 0.5, 4.0),
        "pair_local": draw_pair_local(jax.random.fold_in(key_of[7], 71), 0),
        "pair_other": draw_pair_other(jax.random.fold_in(key_of[7], 71), 0),
        "pair_count": draw_pair_count(jax.random.fold_in(key_of[7], 71), 0),
    }


time_step = 1.0
omega_cycle = 1.2
width_sq = 2.0

def cycle_table(beads):
    bead_index = jnp.arange(beads, dtype=jnp.float32)[:, None]
    mode_index = jnp.arange(beads, dtype=jnp.float32)[None, :]
    middle = beads // 2
    angle = 2.0 * jnp.pi * bead_index * mode_index / beads
    cosine_part = jnp.sqrt(2.0 / beads) * jnp.cos(angle)
    sine_part = jnp.sqrt(2.0 / beads) * jnp.sin(angle)
    edge_part = jnp.sqrt(1.0 / beads) * jnp.cos(jnp.pi * bead_index)
    first = jnp.sqrt(1.0 / beads) * jnp.ones_like(angle)
    table = jnp.where(mode_index == 0, first, jnp.where(mode_index < middle, cosine_part, jnp.where(mode_index == middle, edge_part, sine_part)))
    frequency = 2.0 * omega_cycle * jnp.sin(jnp.pi * jnp.arange(beads, dtype=jnp.float32) / beads)
    return (table, frequency)

def pair_force(left_pos, right_pos, left_charge, right_charge):
    separation = left_pos[..., :, None] - right_pos[..., None, :]
    dist_sq = lax.optimization_barrier(jnp.sum(separation * separation, axis=-3))
    weights = left_charge[..., :, None] * right_charge[..., None, :] * jnp.exp(-dist_sq / (2.0 * width_sq)) / width_sq
    return lax.optimization_barrier(jnp.sum(separation * weights[..., None, :, :], axis=-1))

def propagate(mode_pos, mode_mom, frequency, masses, beads):
    freq_col = frequency[:, None, None]
    mass_row = masses[None, None, :]
    cosine = jnp.cos(freq_col * time_step)
    sine = jnp.sin(freq_col * time_step)
    reach = jnp.where(freq_col > 0, sine / jnp.where(freq_col > 0, freq_col, 1.0), time_step)
    moved_pos = cosine * mode_pos + reach * mode_mom / mass_row
    moved_mom = -mass_row * freq_col * sine * mode_pos + cosine * mode_mom
    spring = lax.optimization_barrier(jnp.sum(0.5 * mass_row * freq_col * freq_col * moved_pos * moved_pos, axis=(0, 1))) / beads
    return (moved_pos, moved_mom, spring)

def reference(positions, momenta, charge, masses, pair_local, pair_other, pair_count):
    tiles_pos = positions.reshape(BEADS, 3, TILES, TILE_ATOMS)
    tile_charge = charge.reshape(TILES, TILE_ATOMS)
    slot_live = (jnp.arange(PAIR_DEV)[None, :] < pair_count[:, None]).astype(jnp.float32).reshape(PAIRS)

    def one_slot(slot_id):
        left_tile = pair_local[slot_id]
        right_tile = pair_other[slot_id]
        left_pos = tiles_pos[:, :, left_tile]
        right_pos = tiles_pos[:, :, right_tile]
        return pair_force(left_pos, right_pos, tile_charge[left_tile] * slot_live[slot_id], tile_charge[right_tile])
    terms = lax.map(one_slot, jnp.arange(PAIRS, dtype=jnp.int32))
    summed = jax.ops.segment_sum(terms, pair_local, num_segments=TILES)
    force = jnp.transpose(summed, (1, 2, 0, 3)).reshape(BEADS, 3, ATOMS)
    kicked = momenta + 0.5 * time_step * force
    table, frequency = cycle_table(BEADS)
    hp = lax.Precision.HIGHEST
    mode_pos = jnp.einsum('jk,jca->kca', table, positions, precision=hp)
    mode_mom = jnp.einsum('jk,jca->kca', table, kicked, precision=hp)
    moved_pos, moved_mom, spring = propagate(mode_pos, mode_mom, frequency, masses, BEADS)
    new_positions = jnp.einsum('jk,kca->jca', table, moved_pos, precision=hp)
    new_momenta = jnp.einsum('jk,kca->jca', table, moved_mom, precision=hp)
    return (new_positions, new_momenta, spring)
```

```python
import functools

import jax
import jax.numpy as jnp
import numpy as np
from jax import lax
from jax.experimental import pallas as pl
from jax.experimental.pallas import tpu as pltpu
from jax.sharding import PartitionSpec as P

time_step = 1.0
omega_cycle = 1.2
width_sq = 2.0
LANES = 128
MESH = pl.DeviceIdType.MESH


def step_matrices(beads, bead_dev):
    j = np.arange(beads, dtype=np.float64)[:, None]
    k = np.arange(beads, dtype=np.float64)[None, :]
    middle = beads // 2
    angle = 2.0 * np.pi * ((j * k) % beads) / beads
    table = np.where(k < middle, np.cos(angle), np.sin(angle)) * np.sqrt(2.0 / beads)
    table[:, 0] = np.sqrt(1.0 / beads)
    table[:, middle] = np.sqrt(1.0 / beads) * (1.0 - 2.0 * (np.arange(beads) % 2))
    freq = 2.0 * omega_cycle * np.sin(np.pi * np.arange(beads) / beads)
    cosine, sine = np.cos(freq * time_step), np.sin(freq * time_step)
    reach = np.where(freq > 0, sine / np.where(freq > 0, freq, 1.0), time_step)
    rows = 3 * bead_dev
    groups = 3 * beads // rows
    order = np.arange(3 * beads).reshape(groups, bead_dev, 3).transpose(0, 2, 1).reshape(-1)

    def spread(matrix):
        return np.kron(matrix, np.eye(3))[order][:, order]

    same = spread((table * cosine) @ table.T)
    drift = spread((table * reach) @ table.T)
    pull = spread((table * (freq * sine)) @ table.T)
    bend_pos = spread((freq * cosine)[:, None] * table.T)
    bend_mom = spread((freq * reach)[:, None] * table.T)

    def mixed(top, bottom):
        both = [top.reshape(groups, rows, -1), bottom.reshape(groups, rows, -1)]
        return np.concatenate(both, axis=1).reshape(2 * rows * groups, -1)

    on_pos = np.concatenate([mixed(same, pull), bend_pos])
    on_mom = np.concatenate([mixed(drift, same), bend_mom])
    return np.stack([on_pos, on_mom]).astype(np.float32)


def kernel(
    beads, bead_count, atom_count,
    local_ref, other_ref, count_ref, pos_ref, mom_ref, charge_ref, mass_ref, mat_ref,
    newp_ref, newm_ref, spring_ref,
    halo_pos, halo_charge, rows_own, cols, acc, full, pos_out, pos_in, kick_out, kick_in,
    back_out, back_in, stack_pos, stack_mom,
    halo_send, halo_recv, pos_send, pos_recv, kick_send, kick_recv, back_send, back_recv,
):
    _, bead_dev, atom_dev = pos_ref.shape
    tile_dev = atom_dev // LANES
    slots = local_ref.shape[0]
    sub = atom_dev // bead_count
    rows = 3 * bead_dev
    me = lax.axis_index("bead")
    here = lax.axis_index("atom")
    up = lax.rem(here + 1, atom_count)
    down = lax.rem(here + atom_count - 1, atom_count)

    barrier = pltpu.get_barrier_semaphore()
    for target in (up, down):
        pl.semaphore_signal(barrier, inc=1, device_id={"atom": target}, device_id_type=MESH)
    for o in range(1, bead_count):
        peer = lax.rem(me + o, bead_count)
        pl.semaphore_signal(barrier, inc=1, device_id={"bead": peer}, device_id_type=MESH)

    def split_rows(ref, out):
        for p in range(bead_count):
            for c in range(3):
                r = slice(bead_dev * c, bead_dev * (c + 1))
                out[p, r, :] = ref[c, :, p * sub : (p + 1) * sub]

    split_rows(pos_ref, pos_out)
    pl.semaphore_wait(barrier, bead_count + 1)

    halo = []
    for side, target in ((0, up), (1, down)):
        for which, (src, dst) in enumerate(((pos_ref, halo_pos), (charge_ref, halo_charge))):
            copy = pltpu.make_async_remote_copy(
                src_ref=src, dst_ref=dst.at[side],
                send_sem=halo_send.at[side, which], recv_sem=halo_recv.at[side, which],
                device_id={"atom": target}, device_id_type=MESH,
            )
            copy.start()
            halo.append(copy)

    def exchange(src, dst, send, recv):
        copies = []
        for o in range(1, bead_count):
            peer = lax.rem(me + o, bead_count)
            copy = pltpu.make_async_remote_copy(
                src_ref=src.at[peer], dst_ref=dst.at[me],
                send_sem=send.at[o], recv_sem=recv.at[o],
                device_id={"bead": peer}, device_id_type=MESH,
            )
            copy.start()
            copies.append(copy)
        return copies

    pos_copies = exchange(pos_out, pos_in, pos_send, pos_recv)

    scale = 0.5 * float(np.sqrt(np.log2(np.e)))

    def lay_tile(pos, charge_row, t, slot, own):
        lanes = slice(t * LANES, (t + 1) * LANES)
        parts = [pos[c, :, lanes] * scale for c in range(3)]
        parts.append(charge_row)
        block = jnp.concatenate(parts, axis=0)
        pad = (-block.shape[0]) % 8
        block = jnp.concatenate([block, jnp.zeros((pad, LANES), jnp.float32)], axis=0)
        if own:
            rows_own[t] = block
        cols[slot] = jnp.transpose(block)

    for t in range(tile_dev):
        lay_tile(pos_ref, charge_ref[t : t + 1, :], t, tile_dev + t, True)
    acc[...] = jnp.zeros_like(acc)
    for copy in halo:
        copy.wait_recv()
    for side, first in ((0, 0), (1, 2 * tile_dev)):
        for t in range(tile_dev):
            lay_tile(
                halo_pos.at[side], halo_charge[side, t : t + 1, :], t, first + t, False
            )

    live_count = count_ref[0]
    base = here * tile_dev
    tiles = tile_dev * atom_count

    def slot_step(s, carry):
        left = lax.rem(local_ref[s], tile_dev)
        right = lax.rem(other_ref[s] - base + tile_dev + tiles, tiles)
        right = jnp.minimum(right, 3 * tile_dev - 1)
        block = rows_own[left]
        xa = [jnp.broadcast_to(block[r : r + 1, :], (8, LANES)) for r in range(rows)]
        total = [jnp.zeros((8, LANES), jnp.float32) for _ in range(rows)]
        for i in range(LANES // 8):
            chunk = cols[right, 8 * i : 8 * i + 8, :]
            charge = jnp.broadcast_to(chunk[:, rows : rows + 1], (8, LANES))
            for b in range(bead_dev):
                at = [bead_dev * c + b for c in range(3)]
                d = [
                    xa[r] - jnp.broadcast_to(chunk[:, r : r + 1], (8, LANES)) for r in at
                ]
                weight = charge * jnp.exp2(-(d[0] * d[0] + d[1] * d[1] + d[2] * d[2]))
                for c in range(3):
                    total[at[c]] = total[at[c]] + weight * d[c]
        summed = jnp.concatenate([jnp.sum(v, axis=0, keepdims=True) for v in total], axis=0)
        live = jnp.where(s < live_count, 2.0 / width_sq * 0.5 / scale, 0.0)
        summed = summed * (block[rows : rows + 1, :] * live)
        for t in range(tile_dev):
            acc[t] = acc[t] + summed * jnp.where(left == t, 1.0, 0.0)
        return carry

    lax.fori_loop(0, slots, slot_step, 0)

    for t in range(tile_dev):
        full[:, t * LANES : (t + 1) * LANES] = acc[t]
    for p in range(bead_count):
        mine = slice(p * sub, (p + 1) * sub)
        for c in range(3):
            r = slice(bead_dev * c, bead_dev * (c + 1))
            kick_out[p, r, :] = mom_ref[c, :, mine] + (0.5 * time_step) * full[r, mine]
    kick_copies = exchange(kick_out, kick_in, kick_send, kick_recv)

    pos_in[me] = pos_out[me]
    kick_in[me] = kick_out[me]
    for copy in pos_copies:
        copy.wait_recv()
    for p in range(bead_count):
        stack_pos[p * rows : (p + 1) * rows, :] = pos_in[p]

    def times(m, x):
        return jnp.dot(
            m, x, precision=lax.Precision.HIGHEST, preferred_element_type=jnp.float32
        )

    from_pos = times(mat_ref[0], stack_pos[...])
    mass = mass_ref[pl.ds(me, 1), :]
    inverse = 1.0 / mass
    for copy in kick_copies:
        copy.wait_recv()
    for p in range(bead_count):
        stack_mom[p * rows : (p + 1) * rows, :] = kick_in[p]
    from_mom = times(mat_ref[1], stack_mom[...])
    both = 2 * rows
    is_pos = lax.broadcasted_iota(jnp.int32, (both, sub), 0) < rows
    weight_pos = jnp.where(is_pos, 1.0, -mass)
    weight_mom = jnp.where(is_pos, inverse, 1.0)
    split = both * bead_count
    bend = from_pos[split:] + from_mom[split:] * inverse
    spring = jnp.sum(bend * bend, axis=0, keepdims=True) * (0.5 * mass) * (1.0 / beads)
    for p in range(bead_count):
        r = slice(p * both, (p + 1) * both)
        back_out[p, :both, :] = from_pos[r] * weight_pos + from_mom[r] * weight_mom
        back_out[p, both : both + 1, :] = spring
    back_copies = exchange(back_out, back_in, back_send, back_recv)
    back_in[me] = back_out[me]
    for copy in back_copies:
        copy.wait_recv()
    for p in range(bead_count):
        mine = slice(p * sub, (p + 1) * sub)
        for c in range(3):
            first = bead_dev * c
            newp_ref[c, :, mine] = back_in[p, first : first + bead_dev, :]
            newm_ref[c, :, mine] = back_in[p, rows + first : rows + first + bead_dev, :]
        spring_ref[:, mine] = back_in[p, both : both + 1, :]
    for copy in halo + pos_copies + kick_copies + back_copies:
        copy.wait_send()


def on_device(positions, momenta, charge, masses, pair_local, pair_other, pair_count):
    positions = jnp.transpose(positions, (1, 0, 2))
    momenta = jnp.transpose(momenta, (1, 0, 2))
    _, bead_dev, atom_dev = positions.shape
    bead_count = lax.axis_size("bead")
    atom_count = lax.axis_size("atom")
    beads = bead_dev * bead_count
    tile_dev = atom_dev // LANES
    sub = atom_dev // bead_count
    rows = 3 * bead_dev
    wide = rows + 1 + (-(rows + 1)) % 8
    f32 = jnp.float32
    vmem = pl.BlockSpec(memory_space=pltpu.VMEM)
    smem = pl.BlockSpec(memory_space=pltpu.SMEM)
    dma = pltpu.SemaphoreType.DMA
    new_positions, new_momenta, spring = pl.pallas_call(
        functools.partial(kernel, beads, bead_count, atom_count),
        out_shape=(
            jax.ShapeDtypeStruct(positions.shape, f32),
            jax.ShapeDtypeStruct(positions.shape, f32),
            jax.ShapeDtypeStruct((1, atom_dev), f32),
        ),
        in_specs=[smem] * 3 + [vmem] * 5,
        out_specs=(vmem, vmem, vmem),
        scratch_shapes=[
            pltpu.VMEM((2,) + positions.shape, f32),
            pltpu.VMEM((2, tile_dev, LANES), f32),
            pltpu.VMEM((tile_dev, wide, LANES), f32),
            pltpu.VMEM((3 * tile_dev, LANES, wide), f32),
            pltpu.VMEM((tile_dev, rows, LANES), f32),
            pltpu.VMEM((rows, atom_dev), f32),
            pltpu.VMEM((bead_count, rows, sub), f32),
            pltpu.VMEM((bead_count, rows, sub), f32),
            pltpu.VMEM((bead_count, rows, sub), f32),
            pltpu.VMEM((bead_count, rows, sub), f32),
            pltpu.VMEM((bead_count, 2 * rows + 1, sub), f32),
            pltpu.VMEM((bead_count, 2 * rows + 1, sub), f32),
            pltpu.VMEM((3 * beads, sub), f32),
            pltpu.VMEM((3 * beads, sub), f32),
            dma((2, 2)),
            dma((2, 2)),
        ]
        + [dma((bead_count,))] * 6,
        compiler_params=pltpu.CompilerParams(collective_id=0, has_side_effects=True),
    )(
        pair_local, pair_other, pair_count, positions, momenta,
        charge.reshape(tile_dev, LANES), masses.reshape(bead_count, sub),
        jnp.asarray(step_matrices(beads, bead_dev)),
    )
    back = (1, 0, 2)
    return (
        jnp.transpose(new_positions, back),
        jnp.transpose(new_momenta, back),
        spring.reshape(atom_dev),
    )


def solution(mesh):
    return jax.shard_map(
        on_device,
        mesh=mesh,
        in_specs=(
            P("bead", None, "atom"),
            P("bead", None, "atom"),
            P("atom"),
            P("atom"),
            P("atom"),
            P("atom"),
            P("atom"),
        ),
        out_specs=(P("bead", None, "atom"), P("bead", None, "atom"), P("atom")),
        check_vma=False,
    )
```

```python
import functools

import jax
import jax.numpy as jnp
import numpy as np
from jax import lax
from jax.experimental import pallas as pl
from jax.experimental.pallas import tpu as pltpu
from jax.sharding import PartitionSpec as P

time_step = 1.0
omega_cycle = 1.2
width_sq = 2.0
LANES = 128
MESH = pl.DeviceIdType.MESH


def step_matrices(beads, bead_dev):
    j = np.arange(beads, dtype=np.float64)[:, None]
    k = np.arange(beads, dtype=np.float64)[None, :]
    middle = beads // 2
    angle = 2.0 * np.pi * ((j * k) % beads) / beads
    table = np.where(k < middle, np.cos(angle), np.sin(angle)) * np.sqrt(2.0 / beads)
    table[:, 0] = np.sqrt(1.0 / beads)
    table[:, middle] = np.sqrt(1.0 / beads) * (1.0 - 2.0 * (np.arange(beads) % 2))
    freq = 2.0 * omega_cycle * np.sin(np.pi * np.arange(beads) / beads)
    cosine, sine = np.cos(freq * time_step), np.sin(freq * time_step)
    reach = np.where(freq > 0, sine / np.where(freq > 0, freq, 1.0), time_step)
    rows = 3 * bead_dev
    groups = 3 * beads // rows
    order = np.arange(3 * beads).reshape(groups, bead_dev, 3).transpose(0, 2, 1).reshape(-1)

    def spread(matrix):
        return np.kron(matrix, np.eye(3))[order][:, order]

    same = spread((table * cosine) @ table.T)
    drift = spread((table * reach) @ table.T)
    pull = spread((table * (freq * sine)) @ table.T)
    bend_pos = spread((freq * cosine)[:, None] * table.T)
    bend_mom = spread((freq * reach)[:, None] * table.T)

    def mixed(top, bottom):
        both = [top.reshape(groups, rows, -1), bottom.reshape(groups, rows, -1)]
        return np.concatenate(both, axis=1).reshape(2 * rows * groups, -1)

    on_pos = np.concatenate([mixed(same, pull), bend_pos])
    on_mom = np.concatenate([mixed(drift, same), bend_mom])
    return np.stack([on_pos, on_mom]).astype(np.float32)


def kernel(
    beads, bead_count, atom_count,
    local_ref, other_ref, count_ref, pos_ref, mom_ref, charge_ref, mass_ref, mat_ref,
    newp_ref, newm_ref, spring_ref,
    halo_pos, halo_charge, own, cols, cols_charge, acc, full, pos_out, pos_in, kick_out, kick_in,
    back_out, back_in, stack_pos, stack_mom,
    halo_send, halo_recv, pos_send, pos_recv, kick_send, kick_recv, back_send, back_recv,
):
    _, bead_dev, atom_dev = pos_ref.shape
    tile_dev = atom_dev // LANES
    slots = local_ref.shape[0]
    sub = atom_dev // bead_count
    rows = 3 * bead_dev
    me = lax.axis_index("bead")
    here = lax.axis_index("atom")
    up = lax.rem(here + 1, atom_count)
    down = lax.rem(here + atom_count - 1, atom_count)

    barrier = pltpu.get_barrier_semaphore()
    for target in (up, down):
        pl.semaphore_signal(barrier, inc=1, device_id={"atom": target}, device_id_type=MESH)
    for o in range(1, bead_count):
        peer = lax.rem(me + o, bead_count)
        pl.semaphore_signal(barrier, inc=1, device_id={"bead": peer}, device_id_type=MESH)

    def split_rows(ref, out):
        for p in range(bead_count):
            for c in range(3):
                r = slice(bead_dev * c, bead_dev * (c + 1))
                out[p, r, :] = ref[c, :, p * sub : (p + 1) * sub]

    split_rows(pos_ref, pos_out)
    pl.semaphore_wait(barrier, bead_count + 1)

    halo = []
    for side, target in ((0, up), (1, down)):
        for which, (src, dst) in enumerate(((pos_ref, halo_pos), (charge_ref, halo_charge))):
            copy = pltpu.make_async_remote_copy(
                src_ref=src, dst_ref=dst.at[side],
                send_sem=halo_send.at[side, which], recv_sem=halo_recv.at[side, which],
                device_id={"atom": target}, device_id_type=MESH,
            )
            copy.start()
            halo.append(copy)

    def exchange(src, dst, send, recv):
        copies = []
        for o in range(1, bead_count):
            peer = lax.rem(me + o, bead_count)
            copy = pltpu.make_async_remote_copy(
                src_ref=src.at[peer], dst_ref=dst.at[me],
                send_sem=send.at[o], recv_sem=recv.at[o],
                device_id={"bead": peer}, device_id_type=MESH,
            )
            copy.start()
            copies.append(copy)
        return copies

    pos_copies = exchange(pos_out, pos_in, pos_send, pos_recv)

    scale = 0.5 * float(np.sqrt(np.log2(np.e)))

    blocks = [bead_dev * c + b for b in range(bead_dev) for c in range(3)]
    tall = rows + (-rows) % 16
    row = lax.rem(lax.broadcasted_iota(jnp.int32, (3 * tall, LANES), 0), tall)
    picks = jnp.concatenate([jnp.where(row == r, -1.0, 0.0) for r in blocks], axis=1)
    picks = picks.astype(jnp.bfloat16)

    def lay_tile(pos, charge_row, t, slot, mine):
        lanes = slice(t * LANES, (t + 1) * LANES)
        block = jnp.concatenate([pos[c, :, lanes] * scale for c in range(3)], axis=0)
        parts = []
        for _ in range(3):
            part = block.astype(jnp.bfloat16).astype(jnp.float32)
            block = block - part
            parts.append(part)
        pad = jnp.zeros((tall - rows, LANES), jnp.float32)
        laid = [v for part in parts for v in (part, pad)]
        laid.append(jnp.ones((tall, LANES), jnp.float32))
        cols[slot] = jnp.transpose(jnp.concatenate(laid, axis=0)).astype(jnp.bfloat16)
        cols_charge[slot] = jnp.transpose(jnp.broadcast_to(charge_row, (8, LANES)))
        if mine:
            flat = [jnp.concatenate([v[r : r + 1] for r in blocks], axis=1) for v in parts]
            flat.append(jnp.zeros((tall - 3, len(blocks) * LANES), jnp.float32))
            own[t, : 3 * tall, :] = picks
            own[t, 3 * tall :, :] = jnp.concatenate(flat, axis=0).astype(jnp.bfloat16)

    for t in range(tile_dev):
        lay_tile(pos_ref, charge_ref[t : t + 1, :], t, tile_dev + t, True)
    acc[...] = jnp.zeros_like(acc)
    for copy in halo:
        copy.wait_recv()
    for side, first in ((0, 0), (1, 2 * tile_dev)):
        for t in range(tile_dev):
            lay_tile(
                halo_pos.at[side], halo_charge[side, t : t + 1, :], t, first + t, False
            )

    live_count = count_ref[0]
    base = here * tile_dev
    tiles = tile_dev * atom_count

    def slot_step(s, carry):
        left = lax.rem(local_ref[s], tile_dev)
        right = lax.rem(other_ref[s] - base + tile_dev + tiles, tiles)
        right = jnp.minimum(right, 3 * tile_dev - 1)
        total = [jnp.zeros((8, LANES), jnp.float32) for _ in range(rows)]
        together = 2
        for first in range(0, bead_dev, together):
            wide = slice(3 * first * LANES, 3 * (first + together) * LANES)
            apart = jnp.dot(
                cols[right], own[left, :, wide], preferred_element_type=jnp.float32
            )
            for i in range(LANES // 8):
                e = slice(8 * i, 8 * i + 8)
                charge = jnp.broadcast_to(cols_charge[right, e, 0:1], (8, LANES))
                for b in range(together):
                    n = [3 * b + c for c in range(3)]
                    d = [apart[e, m * LANES : (m + 1) * LANES] for m in n]
                    weight = charge * jnp.exp2(
                        -(d[0] * d[0] + d[1] * d[1] + d[2] * d[2])
                    )
                    for c in range(3):
                        r = bead_dev * c + first + b
                        total[r] = total[r] + weight * d[c]
        summed = jnp.concatenate([jnp.sum(v, axis=0, keepdims=True) for v in total], axis=0)
        live = jnp.where(s < live_count, 2.0 / width_sq * 0.5 / scale, 0.0)
        summed = summed * (charge_ref[pl.ds(left, 1), :] * live)
        for t in range(tile_dev):
            acc[t] = acc[t] + summed * jnp.where(left == t, 1.0, 0.0)
        return carry

    lax.fori_loop(0, slots, slot_step, 0)

    for t in range(tile_dev):
        full[:, t * LANES : (t + 1) * LANES] = acc[t]
    for p in range(bead_count):
        mine = slice(p * sub, (p + 1) * sub)
        for c in range(3):
            r = slice(bead_dev * c, bead_dev * (c + 1))
            kick_out[p, r, :] = mom_ref[c, :, mine] + (0.5 * time_step) * full[r, mine]
    kick_copies = exchange(kick_out, kick_in, kick_send, kick_recv)

    pos_in[me] = pos_out[me]
    kick_in[me] = kick_out[me]
    for copy in pos_copies:
        copy.wait_recv()
    for p in range(bead_count):
        stack_pos[p * rows : (p + 1) * rows, :] = pos_in[p]

    def times(m, x):
        return jnp.dot(
            m, x, precision=lax.Precision.HIGHEST, preferred_element_type=jnp.float32
        )

    from_pos = times(mat_ref[0], stack_pos[...])
    mass = mass_ref[pl.ds(me, 1), :]
    inverse = 1.0 / mass
    for copy in kick_copies:
        copy.wait_recv()
    for p in range(bead_count):
        stack_mom[p * rows : (p + 1) * rows, :] = kick_in[p]
    from_mom = times(mat_ref[1], stack_mom[...])
    both = 2 * rows
    is_pos = lax.broadcasted_iota(jnp.int32, (both, sub), 0) < rows
    weight_pos = jnp.where(is_pos, 1.0, -mass)
    weight_mom = jnp.where(is_pos, inverse, 1.0)
    split = both * bead_count
    bend = from_pos[split:] + from_mom[split:] * inverse
    spring = jnp.sum(bend * bend, axis=0, keepdims=True) * (0.5 * mass) * (1.0 / beads)
    for p in range(bead_count):
        r = slice(p * both, (p + 1) * both)
        back_out[p, :both, :] = from_pos[r] * weight_pos + from_mom[r] * weight_mom
        back_out[p, both : both + 1, :] = spring
    back_copies = exchange(back_out, back_in, back_send, back_recv)
    back_in[me] = back_out[me]
    for copy in back_copies:
        copy.wait_recv()
    for p in range(bead_count):
        mine = slice(p * sub, (p + 1) * sub)
        for c in range(3):
            first = bead_dev * c
            newp_ref[c, :, mine] = back_in[p, first : first + bead_dev, :]
            newm_ref[c, :, mine] = back_in[p, rows + first : rows + first + bead_dev, :]
        spring_ref[:, mine] = back_in[p, both : both + 1, :]
    for copy in halo + pos_copies + kick_copies + back_copies:
        copy.wait_send()


def on_device(positions, momenta, charge, masses, pair_local, pair_other, pair_count):
    positions = jnp.transpose(positions, (1, 0, 2))
    momenta = jnp.transpose(momenta, (1, 0, 2))
    _, bead_dev, atom_dev = positions.shape
    bead_count = lax.axis_size("bead")
    atom_count = lax.axis_size("atom")
    beads = bead_dev * bead_count
    tile_dev = atom_dev // LANES
    sub = atom_dev // bead_count
    rows = 3 * bead_dev
    deep = 4 * (rows + (-rows) % 16)
    f32 = jnp.float32
    vmem = pl.BlockSpec(memory_space=pltpu.VMEM)
    smem = pl.BlockSpec(memory_space=pltpu.SMEM)
    dma = pltpu.SemaphoreType.DMA
    new_positions, new_momenta, spring = pl.pallas_call(
        functools.partial(kernel, beads, bead_count, atom_count),
        out_shape=(
            jax.ShapeDtypeStruct(positions.shape, f32),
            jax.ShapeDtypeStruct(positions.shape, f32),
            jax.ShapeDtypeStruct((1, atom_dev), f32),
        ),
        in_specs=[smem] * 3 + [vmem] * 5,
        out_specs=(vmem, vmem, vmem),
        scratch_shapes=[
            pltpu.VMEM((2,) + positions.shape, f32),
            pltpu.VMEM((2, tile_dev, LANES), f32),
            pltpu.VMEM((tile_dev, deep, rows * LANES), jnp.bfloat16),
            pltpu.VMEM((3 * tile_dev, LANES, deep), jnp.bfloat16),
            pltpu.VMEM((3 * tile_dev, LANES, 8), f32),
            pltpu.VMEM((tile_dev, rows, LANES), f32),
            pltpu.VMEM((rows, atom_dev), f32),
            pltpu.VMEM((bead_count, rows, sub), f32),
            pltpu.VMEM((bead_count, rows, sub), f32),
            pltpu.VMEM((bead_count, rows, sub), f32),
            pltpu.VMEM((bead_count, rows, sub), f32),
            pltpu.VMEM((bead_count, 2 * rows + 1, sub), f32),
            pltpu.VMEM((bead_count, 2 * rows + 1, sub), f32),
            pltpu.VMEM((3 * beads, sub), f32),
            pltpu.VMEM((3 * beads, sub), f32),
            dma((2, 2)),
            dma((2, 2)),
        ]
        + [dma((bead_count,))] * 6,
        compiler_params=pltpu.CompilerParams(collective_id=0, has_side_effects=True),
    )(
        pair_local, pair_other, pair_count, positions, momenta,
        charge.reshape(tile_dev, LANES), masses.reshape(bead_count, sub),
        jnp.asarray(step_matrices(beads, bead_dev)),
    )
    back = (1, 0, 2)
    return (
        jnp.transpose(new_positions, back),
        jnp.transpose(new_momenta, back),
        spring.reshape(atom_dev),
    )


def solution(mesh):
    return jax.shard_map(
        on_device,
        mesh=mesh,
        in_specs=(
            P("bead", None, "atom"),
            P("bead", None, "atom"),
            P("atom"),
            P("atom"),
            P("atom"),
            P("atom"),
            P("atom"),
        ),
        out_specs=(P("bead", None, "atom"), P("bead", None, "atom"), P("atom")),
        check_vma=False,
    )
```

```python
import functools

import jax
import jax.numpy as jnp
import numpy as np
from jax import lax
from jax.experimental import pallas as pl
from jax.experimental.pallas import tpu as pltpu
from jax.sharding import PartitionSpec as P

time_step = 1.0
omega_cycle = 1.2
width_sq = 2.0
LANES = 128
MESH = pl.DeviceIdType.MESH


def step_matrices(beads, bead_dev):
    j = np.arange(beads, dtype=np.float64)[:, None]
    k = np.arange(beads, dtype=np.float64)[None, :]
    middle = beads // 2
    angle = 2.0 * np.pi * ((j * k) % beads) / beads
    table = np.where(k < middle, np.cos(angle), np.sin(angle)) * np.sqrt(2.0 / beads)
    table[:, 0] = np.sqrt(1.0 / beads)
    table[:, middle] = np.sqrt(1.0 / beads) * (1.0 - 2.0 * (np.arange(beads) % 2))
    freq = 2.0 * omega_cycle * np.sin(np.pi * np.arange(beads) / beads)
    cosine, sine = np.cos(freq * time_step), np.sin(freq * time_step)
    reach = np.where(freq > 0, sine / np.where(freq > 0, freq, 1.0), time_step)
    rows = 3 * bead_dev
    groups = 3 * beads // rows
    order = np.arange(3 * beads).reshape(groups, bead_dev, 3).transpose(0, 2, 1).reshape(-1)

    def spread(matrix):
        return np.kron(matrix, np.eye(3))[order][:, order]

    same = spread((table * cosine) @ table.T)
    drift = spread((table * reach) @ table.T)
    pull = spread((table * (freq * sine)) @ table.T)
    bend_pos = spread((freq * cosine)[:, None] * table.T)
    bend_mom = spread((freq * reach)[:, None] * table.T)

    def mixed(top, bottom):
        both = [top.reshape(groups, rows, -1), bottom.reshape(groups, rows, -1)]
        return np.concatenate(both, axis=1).reshape(2 * rows * groups, -1)

    on_pos = np.concatenate([mixed(same, pull), bend_pos])
    on_mom = np.concatenate([mixed(drift, same), bend_mom])
    return np.stack([on_pos, on_mom]).astype(np.float32)


def kernel(
    beads, bead_count, atom_count,
    local_in, other_in, count_ref, pos_given, mom_given, charge_given, mass_given, mat_given,
    newp_ref, newm_ref, spring_ref,
    local_ref, other_ref, pos_ref, mom_ref, charge_ref, mass_ref, mat_ref, load_sem,
    halo_pos, halo_charge, own, cols, cols_charge, acc, full, pos_out, pos_in, kick_out, kick_in,
    back_out, back_in, stack_pos, stack_mom,
    halo_send, halo_recv, pos_send, pos_recv, kick_send, kick_recv, back_send, back_recv,
):
    _, bead_dev, atom_dev = pos_ref.shape
    tile_dev = atom_dev // LANES
    slots = local_ref.shape[0]
    sub = atom_dev // bead_count
    rows = 3 * bead_dev
    me = lax.axis_index("bead")
    here = lax.axis_index("atom")
    up = lax.rem(here + 1, atom_count)
    down = lax.rem(here + atom_count - 1, atom_count)

    barrier = pltpu.get_barrier_semaphore()
    for target in (up, down):
        pl.semaphore_signal(barrier, inc=1, device_id={"atom": target}, device_id_type=MESH)
    for o in range(1, bead_count):
        peer = lax.rem(me + o, bead_count)
        pl.semaphore_signal(barrier, inc=1, device_id={"bead": peer}, device_id_type=MESH)

    given = (
        (pos_given, pos_ref), (charge_given, charge_ref), (local_in, local_ref),
        (other_in, other_ref), (mom_given, mom_ref),
        (mass_given, mass_ref), (mat_given, mat_ref),
    )
    loads = [
        pltpu.make_async_copy(src, dst, load_sem.at[i]) for i, (src, dst) in enumerate(given)
    ]
    for load in loads:
        load.start()

    def split_rows(ref, out):
        for p in range(bead_count):
            for c in range(3):
                r = slice(bead_dev * c, bead_dev * (c + 1))
                out[p, r, :] = ref[c, :, p * sub : (p + 1) * sub]

    loads[0].wait()
    split_rows(pos_ref, pos_out)
    loads[1].wait()
    pl.semaphore_wait(barrier, bead_count + 1)

    halo = []
    for side, target in ((0, up), (1, down)):
        for which, (src, dst) in enumerate(((pos_ref, halo_pos), (charge_ref, halo_charge))):
            copy = pltpu.make_async_remote_copy(
                src_ref=src, dst_ref=dst.at[side],
                send_sem=halo_send.at[side, which], recv_sem=halo_recv.at[side, which],
                device_id={"atom": target}, device_id_type=MESH,
            )
            copy.start()
            halo.append(copy)

    def exchange(src, dst, send, recv):
        copies = []
        for o in range(1, bead_count):
            peer = lax.rem(me + o, bead_count)
            copy = pltpu.make_async_remote_copy(
                src_ref=src.at[peer], dst_ref=dst.at[me],
                send_sem=send.at[o], recv_sem=recv.at[o],
                device_id={"bead": peer}, device_id_type=MESH,
            )
            copy.start()
            copies.append(copy)
        return copies

    pos_copies = exchange(pos_out, pos_in, pos_send, pos_recv)

    scale = 0.5 * float(np.sqrt(np.log2(np.e)))

    blocks = [bead_dev * c + b for b in range(bead_dev) for c in range(3)]
    tall = rows + (-rows) % 16
    row = lax.rem(lax.broadcasted_iota(jnp.int32, (3 * tall, LANES), 0), tall)
    picks = jnp.concatenate([jnp.where(row == r, -1.0, 0.0) for r in blocks], axis=1)
    picks = picks.astype(jnp.bfloat16)

    def lay_tile(pos, charge_row, t, slot, mine):
        lanes = slice(t * LANES, (t + 1) * LANES)
        block = jnp.concatenate([pos[c, :, lanes] * scale for c in range(3)], axis=0)
        parts = []
        for _ in range(3):
            part = block.astype(jnp.bfloat16).astype(jnp.float32)
            block = block - part
            parts.append(part)
        pad = jnp.zeros((tall - rows, LANES), jnp.float32)
        laid = [v for part in parts for v in (part, pad)]
        laid.append(jnp.ones((tall, LANES), jnp.float32))
        cols[slot] = jnp.transpose(jnp.concatenate(laid, axis=0)).astype(jnp.bfloat16)
        cols_charge[slot] = jnp.transpose(jnp.broadcast_to(charge_row, (8, LANES)))
        if mine:
            flat = [jnp.concatenate([v[r : r + 1] for r in blocks], axis=1) for v in parts]
            flat.append(jnp.zeros((tall - 3, len(blocks) * LANES), jnp.float32))
            own[t, : 3 * tall, :] = picks
            own[t, 3 * tall :, :] = jnp.concatenate(flat, axis=0).astype(jnp.bfloat16)

    for t in range(tile_dev):
        lay_tile(pos_ref, charge_ref[t : t + 1, :], t, tile_dev + t, True)
    acc[...] = jnp.zeros_like(acc)
    for copy in halo:
        copy.wait_recv()
    for side, first in ((0, 0), (1, 2 * tile_dev)):
        for t in range(tile_dev):
            lay_tile(
                halo_pos.at[side], halo_charge[side, t : t + 1, :], t, first + t, False
            )

    for load in loads[2:]:
        load.wait()
    live_count = count_ref[0]
    base = here * tile_dev
    tiles = tile_dev * atom_count

    def slot_step(s):
        left = lax.rem(local_ref[s], tile_dev)
        right = lax.rem(other_ref[s] - base + tile_dev + tiles, tiles)
        right = jnp.minimum(right, 3 * tile_dev - 1)
        total = [jnp.zeros((8, LANES), jnp.float32) for _ in range(rows)]
        together = 2
        for first in range(0, bead_dev, together):
            wide = slice(3 * first * LANES, 3 * (first + together) * LANES)
            apart = jnp.dot(
                cols[right], own[left, :, wide], preferred_element_type=jnp.float32
            )
            for i in range(LANES // 8):
                e = slice(8 * i, 8 * i + 8)
                charge = jnp.broadcast_to(cols_charge[right, e, 0:1], (8, LANES))
                for b in range(together):
                    n = [3 * b + c for c in range(3)]
                    d = [apart[e, m * LANES : (m + 1) * LANES] for m in n]
                    weight = charge * jnp.exp2(
                        -(d[0] * d[0] + d[1] * d[1] + d[2] * d[2])
                    )
                    for c in range(3):
                        r = bead_dev * c + first + b
                        total[r] = total[r] + weight * d[c]
        summed = jnp.concatenate([jnp.sum(v, axis=0, keepdims=True) for v in total], axis=0)
        live = jnp.where(s < live_count, 2.0 / width_sq * 0.5 / scale, 0.0)
        summed = summed * (charge_ref[pl.ds(left, 1), :] * live)
        return left, summed

    together_slots = 2 if slots % 2 == 0 else 1

    def slots_step(i, carry):
        done = [slot_step(i * together_slots + k) for k in range(together_slots)]
        for t in range(tile_dev):
            new = acc[t]
            for left, summed in done:
                new = new + summed * jnp.where(left == t, 1.0, 0.0)
            acc[t] = new
        return carry

    lax.fori_loop(0, slots // together_slots, slots_step, 0)

    for t in range(tile_dev):
        full[:, t * LANES : (t + 1) * LANES] = acc[t]
    for p in range(bead_count):
        mine = slice(p * sub, (p + 1) * sub)
        for c in range(3):
            r = slice(bead_dev * c, bead_dev * (c + 1))
            kick_out[p, r, :] = mom_ref[c, :, mine] + (0.5 * time_step) * full[r, mine]
    kick_copies = exchange(kick_out, kick_in, kick_send, kick_recv)

    pos_in[me] = pos_out[me]
    kick_in[me] = kick_out[me]
    for copy in pos_copies:
        copy.wait_recv()
    for p in range(bead_count):
        stack_pos[p * rows : (p + 1) * rows, :] = pos_in[p]

    def times(m, x):
        return jnp.dot(
            m, x, precision=lax.Precision.HIGHEST, preferred_element_type=jnp.float32
        )

    from_pos = times(mat_ref[0], stack_pos[...])
    mass = mass_ref[pl.ds(me, 1), :]
    inverse = 1.0 / mass
    for copy in kick_copies:
        copy.wait_recv()
    for p in range(bead_count):
        stack_mom[p * rows : (p + 1) * rows, :] = kick_in[p]
    from_mom = times(mat_ref[1], stack_mom[...])
    both = 2 * rows
    is_pos = lax.broadcasted_iota(jnp.int32, (both, sub), 0) < rows
    weight_pos = jnp.where(is_pos, 1.0, -mass)
    weight_mom = jnp.where(is_pos, inverse, 1.0)
    split = both * bead_count
    bend = from_pos[split:] + from_mom[split:] * inverse
    spring = jnp.sum(bend * bend, axis=0, keepdims=True) * (0.5 * mass) * (1.0 / beads)
    for p in range(bead_count):
        r = slice(p * both, (p + 1) * both)
        back_out[p, :both, :] = from_pos[r] * weight_pos + from_mom[r] * weight_mom
        back_out[p, both : both + 1, :] = spring
    back_copies = exchange(back_out, back_in, back_send, back_recv)
    back_in[me] = back_out[me]
    for copy in back_copies:
        copy.wait_recv()
    for p in range(bead_count):
        mine = slice(p * sub, (p + 1) * sub)
        for c in range(3):
            first = bead_dev * c
            newp_ref[c, :, mine] = back_in[p, first : first + bead_dev, :]
            newm_ref[c, :, mine] = back_in[p, rows + first : rows + first + bead_dev, :]
        spring_ref[:, mine] = back_in[p, both : both + 1, :]
    for copy in halo + pos_copies + kick_copies + back_copies:
        copy.wait_send()


def on_device(positions, momenta, charge, masses, pair_local, pair_other, pair_count):
    positions = jnp.transpose(positions, (1, 0, 2))
    momenta = jnp.transpose(momenta, (1, 0, 2))
    _, bead_dev, atom_dev = positions.shape
    bead_count = lax.axis_size("bead")
    atom_count = lax.axis_size("atom")
    beads = bead_dev * bead_count
    tile_dev = atom_dev // LANES
    sub = atom_dev // bead_count
    rows = 3 * bead_dev
    deep = 4 * (rows + (-rows) % 16)
    f32 = jnp.float32
    hbm = pl.BlockSpec(memory_space=pl.ANY)
    vmem = pl.BlockSpec(memory_space=pltpu.VMEM)
    matrices = step_matrices(beads, bead_dev)
    dma = pltpu.SemaphoreType.DMA
    new_positions, new_momenta, spring = pl.pallas_call(
        functools.partial(kernel, beads, bead_count, atom_count),
        out_shape=(
            jax.ShapeDtypeStruct(positions.shape, f32),
            jax.ShapeDtypeStruct(positions.shape, f32),
            jax.ShapeDtypeStruct((1, atom_dev), f32),
        ),
        in_specs=[hbm, hbm, pl.BlockSpec(memory_space=pltpu.SMEM)] + [hbm] * 5,
        out_specs=(vmem, vmem, vmem),
        scratch_shapes=[
            pltpu.SMEM(pair_local.shape, jnp.int32),
            pltpu.SMEM(pair_other.shape, jnp.int32),
            pltpu.VMEM(positions.shape, f32),
            pltpu.VMEM(positions.shape, f32),
            pltpu.VMEM((tile_dev, LANES), f32),
            pltpu.VMEM((bead_count, sub), f32),
            pltpu.VMEM(matrices.shape, f32),
            dma((7,)),
            pltpu.VMEM((2,) + positions.shape, f32),
            pltpu.VMEM((2, tile_dev, LANES), f32),
            pltpu.VMEM((tile_dev, deep, rows * LANES), jnp.bfloat16),
            pltpu.VMEM((3 * tile_dev, LANES, deep), jnp.bfloat16),
            pltpu.VMEM((3 * tile_dev, LANES, 8), f32),
            pltpu.VMEM((tile_dev, rows, LANES), f32),
            pltpu.VMEM((rows, atom_dev), f32),
            pltpu.VMEM((bead_count, rows, sub), f32),
            pltpu.VMEM((bead_count, rows, sub), f32),
            pltpu.VMEM((bead_count, rows, sub), f32),
            pltpu.VMEM((bead_count, rows, sub), f32),
            pltpu.VMEM((bead_count, 2 * rows + 1, sub), f32),
            pltpu.VMEM((bead_count, 2 * rows + 1, sub), f32),
            pltpu.VMEM((3 * beads, sub), f32),
            pltpu.VMEM((3 * beads, sub), f32),
            dma((2, 2)),
            dma((2, 2)),
        ]
        + [dma((bead_count,))] * 6,
        compiler_params=pltpu.CompilerParams(collective_id=0, has_side_effects=True),
    )(
        pair_local, pair_other, pair_count, positions, momenta,
        charge.reshape(tile_dev, LANES), masses.reshape(bead_count, sub),
        jnp.asarray(matrices),
    )
    back = (1, 0, 2)
    return (
        jnp.transpose(new_positions, back),
        jnp.transpose(new_momenta, back),
        spring.reshape(atom_dev),
    )


def solution(mesh):
    return jax.shard_map(
        on_device,
        mesh=mesh,
        in_specs=(
            P("bead", None, "atom"),
            P("bead", None, "atom"),
            P("atom"),
            P("atom"),
            P("atom"),
            P("atom"),
            P("atom"),
        ),
        out_specs=(P("bead", None, "atom"), P("bead", None, "atom"), P("atom")),
        check_vma=False,
    )
```

```python
import functools

import jax
import jax.numpy as jnp
import numpy as np
from jax import lax
from jax.experimental import pallas as pl
from jax.experimental.pallas import tpu as pltpu
from jax.sharding import PartitionSpec as P

time_step = 1.0
omega_cycle = 1.2
width_sq = 2.0
LANES = 128
MESH = pl.DeviceIdType.MESH


def step_matrices(beads, bead_dev):
    j = np.arange(beads, dtype=np.float64)[:, None]
    k = np.arange(beads, dtype=np.float64)[None, :]
    middle = beads // 2
    angle = 2.0 * np.pi * ((j * k) % beads) / beads
    table = np.where(k < middle, np.cos(angle), np.sin(angle)) * np.sqrt(2.0 / beads)
    table[:, 0] = np.sqrt(1.0 / beads)
    table[:, middle] = np.sqrt(1.0 / beads) * (1.0 - 2.0 * (np.arange(beads) % 2))
    freq = 2.0 * omega_cycle * np.sin(np.pi * np.arange(beads) / beads)
    cosine, sine = np.cos(freq * time_step), np.sin(freq * time_step)
    reach = np.where(freq > 0, sine / np.where(freq > 0, freq, 1.0), time_step)
    rows = 3 * bead_dev
    groups = 3 * beads // rows
    order = np.arange(3 * beads).reshape(groups, bead_dev, 3).transpose(0, 2, 1).reshape(-1)

    def spread(matrix):
        return np.kron(matrix, np.eye(3))[order][:, order]

    same = spread((table * cosine) @ table.T)
    drift = spread((table * reach) @ table.T)
    pull = spread((table * (freq * sine)) @ table.T)
    bend_pos = spread((freq * cosine)[:, None] * table.T)
    bend_mom = spread((freq * reach)[:, None] * table.T)

    def mixed(top, bottom):
        both = [top.reshape(groups, rows, -1), bottom.reshape(groups, rows, -1)]
        return np.concatenate(both, axis=1).reshape(2 * rows * groups, -1)

    on_pos = np.concatenate([mixed(same, pull), bend_pos])
    on_mom = np.concatenate([mixed(drift, same), bend_mom])
    return np.stack([on_pos, on_mom]).astype(np.float32)


def kernel(
    beads, bead_count, atom_count,
    local_in, other_in, count_ref, pos_given, mom_given, charge_given, mass_given, mat_given,
    newp_ref, newm_ref, spring_ref,
    local_ref, other_ref, pos_ref, mom_ref, charge_ref, mass_ref, mat_ref, load_sem,
    halo_pos, halo_charge, own, cols, cols_charge, acc, full, pos_out, pos_in, kick_out, kick_in,
    back_out, back_in, stack_pos, stack_mom,
    halo_send, halo_recv, pos_send, pos_recv, kick_send, kick_recv, back_send, back_recv,
):
    _, bead_dev, atom_dev = pos_ref.shape
    tile_dev = atom_dev // LANES
    slots = local_ref.shape[0]
    sub = atom_dev // bead_count
    rows = 3 * bead_dev
    me = lax.axis_index("bead")
    here = lax.axis_index("atom")
    up = lax.rem(here + 1, atom_count)
    down = lax.rem(here + atom_count - 1, atom_count)

    barrier = pltpu.get_barrier_semaphore()
    for target in (up, down):
        pl.semaphore_signal(barrier, inc=1, device_id={"atom": target}, device_id_type=MESH)
    for o in range(1, bead_count):
        peer = lax.rem(me + o, bead_count)
        pl.semaphore_signal(barrier, inc=1, device_id={"bead": peer}, device_id_type=MESH)

    given = (
        (pos_given, pos_ref), (charge_given, charge_ref), (local_in, local_ref),
        (other_in, other_ref), (mom_given, mom_ref),
        (mass_given, mass_ref), (mat_given, mat_ref),
    )
    loads = [
        pltpu.make_async_copy(src, dst, load_sem.at[i]) for i, (src, dst) in enumerate(given)
    ]
    for load in loads:
        load.start()

    def split_rows(ref, out):
        for p in range(bead_count):
            for c in range(3):
                r = slice(bead_dev * c, bead_dev * (c + 1))
                out[p, r, :] = ref[c, :, p * sub : (p + 1) * sub]

    loads[0].wait()
    split_rows(pos_ref, pos_out)
    loads[1].wait()
    pl.semaphore_wait(barrier, bead_count + 1)

    halo = []
    for side, target in ((0, up), (1, down)):
        for which, (src, dst) in enumerate(((pos_ref, halo_pos), (charge_ref, halo_charge))):
            copy = pltpu.make_async_remote_copy(
                src_ref=src, dst_ref=dst.at[side],
                send_sem=halo_send.at[side, which], recv_sem=halo_recv.at[side, which],
                device_id={"atom": target}, device_id_type=MESH,
            )
            copy.start()
            halo.append(copy)

    def exchange(src, dst, send, recv):
        copies = []
        for o in range(1, bead_count):
            peer = lax.rem(me + o, bead_count)
            copy = pltpu.make_async_remote_copy(
                src_ref=src.at[peer], dst_ref=dst.at[me],
                send_sem=send.at[o], recv_sem=recv.at[o],
                device_id={"bead": peer}, device_id_type=MESH,
            )
            copy.start()
            copies.append(copy)
        return copies

    pos_copies = exchange(pos_out, pos_in, pos_send, pos_recv)

    scale = 0.5 * float(np.sqrt(np.log2(np.e)))

    blocks = [bead_dev * c + b for b in range(bead_dev) for c in range(3)]
    tall = rows + (-rows) % 16
    row = lax.rem(lax.broadcasted_iota(jnp.int32, (3 * tall, LANES), 0), tall)
    picks = jnp.concatenate([jnp.where(row == r, -1.0, 0.0) for r in blocks], axis=1)
    picks = picks.astype(jnp.bfloat16)

    def lay_tile(pos, charge_row, t, slot, mine):
        lanes = slice(t * LANES, (t + 1) * LANES)
        block = jnp.concatenate([pos[c, :, lanes] * scale for c in range(3)], axis=0)
        parts = []
        for _ in range(3):
            part = block.astype(jnp.bfloat16).astype(jnp.float32)
            block = block - part
            parts.append(part)
        pad = jnp.zeros((tall - rows, LANES), jnp.float32)
        laid = [v for part in parts for v in (part, pad)]
        laid.append(jnp.ones((tall, LANES), jnp.float32))
        cols[slot] = jnp.transpose(jnp.concatenate(laid, axis=0)).astype(jnp.bfloat16)
        cols_charge[slot] = jnp.transpose(jnp.broadcast_to(charge_row, (8, LANES)))
        if mine:
            flat = [jnp.concatenate([v[r : r + 1] for r in blocks], axis=1) for v in parts]
            flat.append(jnp.zeros((tall - 3, len(blocks) * LANES), jnp.float32))
            own[t, : 3 * tall, :] = picks
            own[t, 3 * tall :, :] = jnp.concatenate(flat, axis=0).astype(jnp.bfloat16)

    for t in range(tile_dev):
        lay_tile(pos_ref, charge_ref[t : t + 1, :], t, tile_dev + t, True)
    acc[...] = jnp.zeros_like(acc)
    for copy in halo:
        copy.wait_recv()
    for side, first in ((0, 0), (1, 2 * tile_dev)):
        for t in range(tile_dev):
            lay_tile(
                halo_pos.at[side], halo_charge[side, t : t + 1, :], t, first + t, False
            )

    for load in loads[2:]:
        load.wait()
    live_count = count_ref[0]
    base = here * tile_dev
    tiles = tile_dev * atom_count

    def slot_step(s):
        left = lax.rem(local_ref[s], tile_dev)
        right = lax.rem(other_ref[s] - base + tile_dev + tiles, tiles)
        right = jnp.minimum(right, 3 * tile_dev - 1)
        total = [jnp.zeros((8, LANES), jnp.float32) for _ in range(rows)]
        together = 2
        for first in range(0, bead_dev, together):
            wide = slice(3 * first * LANES, 3 * (first + together) * LANES)
            apart = jnp.dot(
                cols[right], own[left, :, wide], preferred_element_type=jnp.float32
            )
            for i in range(LANES // 8):
                e = slice(8 * i, 8 * i + 8)
                charge = jnp.broadcast_to(cols_charge[right, e, 0:1], (8, LANES))
                for b in range(together):
                    n = [3 * b + c for c in range(3)]
                    d = [apart[e, m * LANES : (m + 1) * LANES] for m in n]
                    weight = charge * jnp.exp2(
                        -(d[0] * d[0] + d[1] * d[1] + d[2] * d[2])
                    )
                    for c in range(3):
                        r = bead_dev * c + first + b
                        total[r] = total[r] + weight * d[c]
        summed = jnp.concatenate([jnp.sum(v, axis=0, keepdims=True) for v in total], axis=0)
        live = jnp.where(s < live_count, 2.0 / width_sq * 0.5 / scale, 0.0)
        summed = summed * (charge_ref[pl.ds(left, 1), :] * live)
        return left, summed

    together_slots = 2 if slots % 2 == 0 else 1

    def slots_step(i, carry):
        done = [slot_step(i * together_slots + k) for k in range(together_slots)]
        for t in range(tile_dev):
            new = acc[t]
            for left, summed in done:
                new = new + summed * jnp.where(left == t, 1.0, 0.0)
            acc[t] = new
        return carry

    lax.fori_loop(0, slots // together_slots, slots_step, 0)

    for t in range(tile_dev):
        full[:, t * LANES : (t + 1) * LANES] = acc[t]
    for p in range(bead_count):
        mine = slice(p * sub, (p + 1) * sub)
        for c in range(3):
            r = slice(bead_dev * c, bead_dev * (c + 1))
            kick_out[p, r, :] = mom_ref[c, :, mine] + (0.5 * time_step) * full[r, mine]
    kick_copies = exchange(kick_out, kick_in, kick_send, kick_recv)

    pos_in[me] = pos_out[me]
    kick_in[me] = kick_out[me]
    for copy in pos_copies:
        copy.wait_recv()
    for p in range(bead_count):
        stack_pos[p * rows : (p + 1) * rows, :] = pos_in[p]

    def times(m, x):
        return jnp.dot(
            m, x, precision=lax.Precision.HIGHEST, preferred_element_type=jnp.float32
        )

    from_pos = times(mat_ref[0], stack_pos[...])
    mass = mass_ref[pl.ds(me, 1), :]
    inverse = 1.0 / mass
    for copy in kick_copies:
        copy.wait_recv()
    for p in range(bead_count):
        stack_mom[p * rows : (p + 1) * rows, :] = kick_in[p]
    from_mom = times(mat_ref[1], stack_mom[...])
    both = 2 * rows
    is_pos = lax.broadcasted_iota(jnp.int32, (both, sub), 0) < rows
    weight_pos = jnp.where(is_pos, 1.0, -mass)
    weight_mom = jnp.where(is_pos, inverse, 1.0)
    split = both * bead_count
    bend = from_pos[split:] + from_mom[split:] * inverse
    spring = jnp.sum(bend * bend, axis=0, keepdims=True) * (0.5 * mass) * (1.0 / beads)
    for p in range(bead_count):
        r = slice(p * both, (p + 1) * both)
        back_out[p, :both, :] = from_pos[r] * weight_pos + from_mom[r] * weight_mom
        back_out[p, both : both + 1, :] = spring
    back_copies = exchange(back_out, back_in, back_send, back_recv)
    back_in[me] = back_out[me]
    for copy in back_copies:
        copy.wait_recv()
    for p in range(bead_count):
        mine = slice(p * sub, (p + 1) * sub)
        for c in range(3):
            first = bead_dev * c
            newp_ref[c, :, mine] = back_in[p, first : first + bead_dev, :]
            newm_ref[c, :, mine] = back_in[p, rows + first : rows + first + bead_dev, :]
        spring_ref[:, mine] = back_in[p, both : both + 1, :]
    for copy in halo + pos_copies + kick_copies + back_copies:
        copy.wait_send()


def hand_over(*refs):
    half = len(refs) // 2
    for src, dst in zip(refs[:half], refs[half:]):
        dst[...] = src[...]


def on_device(positions, momenta, charge, masses, pair_local, pair_other, pair_count):
    positions = jnp.transpose(positions, (1, 0, 2))
    momenta = jnp.transpose(momenta, (1, 0, 2))
    _, bead_dev, atom_dev = positions.shape
    bead_count = lax.axis_size("bead")
    atom_count = lax.axis_size("atom")
    beads = bead_dev * bead_count
    tile_dev = atom_dev // LANES
    sub = atom_dev // bead_count
    rows = 3 * bead_dev
    deep = 4 * (rows + (-rows) % 16)
    f32 = jnp.float32
    hbm = pl.BlockSpec(memory_space=pl.ANY)
    vmem = pl.BlockSpec(memory_space=pltpu.VMEM)
    matrices = step_matrices(beads, bead_dev)
    dma = pltpu.SemaphoreType.DMA
    new_positions, new_momenta, spring = pl.pallas_call(
        functools.partial(kernel, beads, bead_count, atom_count),
        out_shape=(
            jax.ShapeDtypeStruct(positions.shape, f32),
            jax.ShapeDtypeStruct(positions.shape, f32),
            jax.ShapeDtypeStruct((1, atom_dev), f32),
        ),
        in_specs=[hbm, hbm, pl.BlockSpec(memory_space=pltpu.SMEM)] + [hbm] * 5,
        out_specs=(vmem, vmem, vmem),
        scratch_shapes=[
            pltpu.SMEM(pair_local.shape, jnp.int32),
            pltpu.SMEM(pair_other.shape, jnp.int32),
            pltpu.VMEM(positions.shape, f32),
            pltpu.VMEM(positions.shape, f32),
            pltpu.VMEM((tile_dev, LANES), f32),
            pltpu.VMEM((bead_count, sub), f32),
            pltpu.VMEM(matrices.shape, f32),
            dma((7,)),
            pltpu.VMEM((2,) + positions.shape, f32),
            pltpu.VMEM((2, tile_dev, LANES), f32),
            pltpu.VMEM((tile_dev, deep, rows * LANES), jnp.bfloat16),
            pltpu.VMEM((3 * tile_dev, LANES, deep), jnp.bfloat16),
            pltpu.VMEM((3 * tile_dev, LANES, 8), f32),
            pltpu.VMEM((tile_dev, rows, LANES), f32),
            pltpu.VMEM((rows, atom_dev), f32),
            pltpu.VMEM((bead_count, rows, sub), f32),
            pltpu.VMEM((bead_count, rows, sub), f32),
            pltpu.VMEM((bead_count, rows, sub), f32),
            pltpu.VMEM((bead_count, rows, sub), f32),
            pltpu.VMEM((bead_count, 2 * rows + 1, sub), f32),
            pltpu.VMEM((bead_count, 2 * rows + 1, sub), f32),
            pltpu.VMEM((3 * beads, sub), f32),
            pltpu.VMEM((3 * beads, sub), f32),
            dma((2, 2)),
            dma((2, 2)),
        ]
        + [dma((bead_count,))] * 6,
        compiler_params=pltpu.CompilerParams(collective_id=0, has_side_effects=True),
    )(
        pair_local, pair_other, pair_count, positions, momenta,
        charge.reshape(tile_dev, LANES), masses.reshape(bead_count, sub),
        jnp.asarray(matrices),
    )
    results = (new_positions, new_momenta, spring)
    new_positions, new_momenta, spring = pl.pallas_call(
        hand_over,
        out_shape=tuple(jax.ShapeDtypeStruct(v.shape, f32) for v in results),
        in_specs=[vmem] * 3,
        out_specs=(vmem,) * 3,
    )(*results)
    back = (1, 0, 2)
    return (
        jnp.transpose(new_positions, back),
        jnp.transpose(new_momenta, back),
        spring.reshape(atom_dev),
    )


def solution(mesh):
    return jax.shard_map(
        on_device,
        mesh=mesh,
        in_specs=(
            P("bead", None, "atom"),
            P("bead", None, "atom"),
            P("atom"),
            P("atom"),
            P("atom"),
            P("atom"),
            P("atom"),
        ),
        out_specs=(P("bead", None, "atom"), P("bead", None, "atom"), P("atom")),
        check_vma=False,
    )
```

```python
import functools

import jax
import jax.numpy as jnp
import numpy as np
from jax import lax
from jax.experimental import pallas as pl
from jax.experimental.pallas import tpu as pltpu
from jax.sharding import PartitionSpec as P

time_step = 1.0
omega_cycle = 1.2
width_sq = 2.0
LANES = 128
MESH = pl.DeviceIdType.MESH


def step_matrices(beads, bead_dev):
    j = np.arange(beads, dtype=np.float64)[:, None]
    k = np.arange(beads, dtype=np.float64)[None, :]
    middle = beads // 2
    angle = 2.0 * np.pi * ((j * k) % beads) / beads
    table = np.where(k < middle, np.cos(angle), np.sin(angle)) * np.sqrt(2.0 / beads)
    table[:, 0] = np.sqrt(1.0 / beads)
    table[:, middle] = np.sqrt(1.0 / beads) * (1.0 - 2.0 * (np.arange(beads) % 2))
    freq = 2.0 * omega_cycle * np.sin(np.pi * np.arange(beads) / beads)
    cosine, sine = np.cos(freq * time_step), np.sin(freq * time_step)
    reach = np.where(freq > 0, sine / np.where(freq > 0, freq, 1.0), time_step)
    rows = 3 * bead_dev
    groups = 3 * beads // rows
    order = np.arange(3 * beads).reshape(groups, bead_dev, 3).transpose(0, 2, 1).reshape(-1)

    def spread(matrix):
        return np.kron(matrix, np.eye(3))[order][:, order]

    same = spread((table * cosine) @ table.T)
    drift = spread((table * reach) @ table.T)
    pull = spread((table * (freq * sine)) @ table.T)
    bend_pos = spread((freq * cosine)[:, None] * table.T)
    bend_mom = spread((freq * reach)[:, None] * table.T)

    def mixed(top, bottom):
        both = [top.reshape(groups, rows, -1), bottom.reshape(groups, rows, -1)]
        return np.concatenate(both, axis=1).reshape(2 * rows * groups, -1)

    on_pos = np.concatenate([mixed(same, pull), bend_pos])
    on_mom = np.concatenate([mixed(drift, same), bend_mom])
    return np.stack([on_pos, on_mom]).astype(np.float32)


def kernel(
    beads, bead_count, atom_count,
    local_in, other_in, count_ref, pos_given, mom_given, charge_given, mass_given, mat_given,
    newp_ref, newm_ref, spring_ref,
    local_ref, other_ref, pos_ref, mom_ref, charge_ref, mass_ref, mat_ref, load_sem,
    halo_pos, halo_charge, own, cols, cols_charge, acc, full, pos_out, pos_in, kick_out, kick_in,
    back_out, back_in, stack_pos, stack_mom,
    halo_send, halo_recv, pos_send, pos_recv, kick_send, kick_recv, back_send, back_recv,
):
    _, bead_dev, atom_dev = pos_ref.shape
    tile_dev = atom_dev // LANES
    slots = local_ref.shape[0]
    sub = atom_dev // bead_count
    rows = 3 * bead_dev
    me = lax.axis_index("bead")
    here = lax.axis_index("atom")
    up = lax.rem(here + 1, atom_count)
    down = lax.rem(here + atom_count - 1, atom_count)

    barrier = pltpu.get_barrier_semaphore()
    for target in (up, down):
        pl.semaphore_signal(barrier, inc=1, device_id={"atom": target}, device_id_type=MESH)
    for o in range(1, bead_count):
        peer = lax.rem(me + o, bead_count)
        pl.semaphore_signal(barrier, inc=1, device_id={"bead": peer}, device_id_type=MESH)

    given = (
        (pos_given, pos_ref), (charge_given, charge_ref), (local_in, local_ref),
        (other_in, other_ref), (mom_given, mom_ref),
        (mass_given, mass_ref), (mat_given, mat_ref),
    )
    loads = [
        pltpu.make_async_copy(src, dst, load_sem.at[i]) for i, (src, dst) in enumerate(given)
    ]
    for load in loads:
        load.start()

    def split_rows(ref, out):
        for p in range(bead_count):
            for c in range(3):
                r = slice(bead_dev * c, bead_dev * (c + 1))
                out[p, r, :] = ref[c, :, p * sub : (p + 1) * sub]

    loads[0].wait()
    split_rows(pos_ref, pos_out)
    loads[1].wait()
    pl.semaphore_wait(barrier, bead_count + 1)

    halo = []
    for side, target in ((0, up), (1, down)):
        for which, (src, dst) in enumerate(((pos_ref, halo_pos), (charge_ref, halo_charge))):
            copy = pltpu.make_async_remote_copy(
                src_ref=src, dst_ref=dst.at[side],
                send_sem=halo_send.at[side, which], recv_sem=halo_recv.at[side, which],
                device_id={"atom": target}, device_id_type=MESH,
            )
            copy.start()
            halo.append(copy)

    def exchange(src, dst, send, recv):
        copies = []
        for o in range(1, bead_count):
            peer = lax.rem(me + o, bead_count)
            copy = pltpu.make_async_remote_copy(
                src_ref=src.at[peer], dst_ref=dst.at[me],
                send_sem=send.at[o], recv_sem=recv.at[o],
                device_id={"bead": peer}, device_id_type=MESH,
            )
            copy.start()
            copies.append(copy)
        return copies

    pos_copies = exchange(pos_out, pos_in, pos_send, pos_recv)

    scale = 0.5 * float(np.sqrt(np.log2(np.e)))

    blocks = [bead_dev * c + b for b in range(bead_dev) for c in range(3)]
    tall = rows + (-rows) % 16
    row = lax.rem(lax.broadcasted_iota(jnp.int32, (3 * tall, LANES), 0), tall)
    picks = jnp.concatenate([jnp.where(row == r, -1.0, 0.0) for r in blocks], axis=1)
    picks = picks.astype(jnp.bfloat16)

    def lay_tile(pos, charge_row, t, slot, mine):
        lanes = slice(t * LANES, (t + 1) * LANES)
        block = jnp.concatenate([pos[c, :, lanes] * scale for c in range(3)], axis=0)
        parts = []
        for _ in range(3):
            part = block.astype(jnp.bfloat16).astype(jnp.float32)
            block = block - part
            parts.append(part)
        pad = jnp.zeros((tall - rows, LANES), jnp.float32)
        laid = [v for part in parts for v in (part, pad)]
        laid.append(jnp.ones((tall, LANES), jnp.float32))
        cols[slot] = jnp.transpose(jnp.concatenate(laid, axis=0)).astype(jnp.bfloat16)
        cols_charge[slot] = jnp.transpose(jnp.broadcast_to(charge_row, (8, LANES)))
        if mine:
            flat = [jnp.concatenate([v[r : r + 1] for r in blocks], axis=1) for v in parts]
            flat.append(jnp.zeros((tall - 3, len(blocks) * LANES), jnp.float32))
            own[t, : 3 * tall, :] = picks
            own[t, 3 * tall :, :] = jnp.concatenate(flat, axis=0).astype(jnp.bfloat16)

    for t in range(tile_dev):
        lay_tile(pos_ref, charge_ref[t : t + 1, :], t, tile_dev + t, True)
    acc[...] = jnp.zeros_like(acc)
    for copy in halo:
        copy.wait_recv()
    for side, first in ((0, 0), (1, 2 * tile_dev)):
        for t in range(tile_dev):
            lay_tile(
                halo_pos.at[side], halo_charge[side, t : t + 1, :], t, first + t, False
            )

    for load in loads[2:]:
        load.wait()
    live_count = count_ref[0]
    base = here * tile_dev
    tiles = tile_dev * atom_count

    def slot_step(s):
        left = lax.rem(local_ref[s], tile_dev)
        right = lax.rem(other_ref[s] - base + tile_dev + tiles, tiles)
        right = jnp.minimum(right, 3 * tile_dev - 1)
        total = [jnp.zeros((8, LANES), jnp.float32) for _ in range(rows)]
        together = 2
        for first in range(0, bead_dev, together):
            wide = slice(3 * first * LANES, 3 * (first + together) * LANES)
            apart = jnp.dot(
                cols[right], own[left, :, wide], preferred_element_type=jnp.float32
            )
            for i in range(LANES // 8):
                e = slice(8 * i, 8 * i + 8)
                charge = jnp.broadcast_to(cols_charge[right, e, 0:1], (8, LANES))
                for b in range(together):
                    n = [3 * b + c for c in range(3)]
                    d = [apart[e, m * LANES : (m + 1) * LANES] for m in n]
                    weight = charge * jnp.exp2(
                        -(d[0] * d[0] + d[1] * d[1] + d[2] * d[2])
                    )
                    for c in range(3):
                        r = bead_dev * c + first + b
                        total[r] = total[r] + weight * d[c]
        summed = jnp.concatenate([jnp.sum(v, axis=0, keepdims=True) for v in total], axis=0)
        live = jnp.where(s < live_count, 2.0 / width_sq * 0.5 / scale, 0.0)
        summed = summed * (charge_ref[pl.ds(left, 1), :] * live)
        return left, summed

    together_slots = 4 if slots % 4 == 0 else 1

    def slots_step(i, carry):
        done = [slot_step(i * together_slots + k) for k in range(together_slots)]
        for t in range(tile_dev):
            new = acc[t]
            for left, summed in done:
                new = new + summed * jnp.where(left == t, 1.0, 0.0)
            acc[t] = new
        return carry

    lax.fori_loop(0, slots // together_slots, slots_step, 0)

    for t in range(tile_dev):
        full[:, t * LANES : (t + 1) * LANES] = acc[t]
    for p in range(bead_count):
        mine = slice(p * sub, (p + 1) * sub)
        for c in range(3):
            r = slice(bead_dev * c, bead_dev * (c + 1))
            kick_out[p, r, :] = mom_ref[c, :, mine] + (0.5 * time_step) * full[r, mine]
    kick_copies = exchange(kick_out, kick_in, kick_send, kick_recv)

    pos_in[me] = pos_out[me]
    kick_in[me] = kick_out[me]
    for copy in pos_copies:
        copy.wait_recv()
    for p in range(bead_count):
        stack_pos[p * rows : (p + 1) * rows, :] = pos_in[p]

    def times(m, x):
        return jnp.dot(
            m, x, precision=lax.Precision.HIGHEST, preferred_element_type=jnp.float32
        )

    from_pos = times(mat_ref[0], stack_pos[...])
    mass = mass_ref[pl.ds(me, 1), :]
    inverse = 1.0 / mass
    for copy in kick_copies:
        copy.wait_recv()
    for p in range(bead_count):
        stack_mom[p * rows : (p + 1) * rows, :] = kick_in[p]
    from_mom = times(mat_ref[1], stack_mom[...])
    both = 2 * rows
    is_pos = lax.broadcasted_iota(jnp.int32, (both, sub), 0) < rows
    weight_pos = jnp.where(is_pos, 1.0, -mass)
    weight_mom = jnp.where(is_pos, inverse, 1.0)
    split = both * bead_count
    bend = from_pos[split:] + from_mom[split:] * inverse
    spring = jnp.sum(bend * bend, axis=0, keepdims=True) * (0.5 * mass) * (1.0 / beads)
    for p in range(bead_count):
        r = slice(p * both, (p + 1) * both)
        back_out[p, :both, :] = from_pos[r] * weight_pos + from_mom[r] * weight_mom
        back_out[p, both : both + 1, :] = spring
    back_copies = exchange(back_out, back_in, back_send, back_recv)
    back_in[me] = back_out[me]
    for copy in back_copies:
        copy.wait_recv()
    for p in range(bead_count):
        mine = slice(p * sub, (p + 1) * sub)
        for c in range(3):
            first = bead_dev * c
            newp_ref[c, :, mine] = back_in[p, first : first + bead_dev, :]
            newm_ref[c, :, mine] = back_in[p, rows + first : rows + first + bead_dev, :]
        spring_ref[:, mine] = back_in[p, both : both + 1, :]
    for copy in halo + pos_copies + kick_copies + back_copies:
        copy.wait_send()


def hand_over(*refs):
    half = len(refs) // 2
    for src, dst in zip(refs[:half], refs[half:]):
        dst[...] = src[...]


def on_device(positions, momenta, charge, masses, pair_local, pair_other, pair_count):
    positions = jnp.transpose(positions, (1, 0, 2))
    momenta = jnp.transpose(momenta, (1, 0, 2))
    _, bead_dev, atom_dev = positions.shape
    bead_count = lax.axis_size("bead")
    atom_count = lax.axis_size("atom")
    beads = bead_dev * bead_count
    tile_dev = atom_dev // LANES
    sub = atom_dev // bead_count
    rows = 3 * bead_dev
    deep = 4 * (rows + (-rows) % 16)
    f32 = jnp.float32
    hbm = pl.BlockSpec(memory_space=pl.ANY)
    vmem = pl.BlockSpec(memory_space=pltpu.VMEM)
    matrices = step_matrices(beads, bead_dev)
    dma = pltpu.SemaphoreType.DMA
    new_positions, new_momenta, spring = pl.pallas_call(
        functools.partial(kernel, beads, bead_count, atom_count),
        out_shape=(
            jax.ShapeDtypeStruct(positions.shape, f32),
            jax.ShapeDtypeStruct(positions.shape, f32),
            jax.ShapeDtypeStruct((1, atom_dev), f32),
        ),
        in_specs=[hbm, hbm, pl.BlockSpec(memory_space=pltpu.SMEM)] + [hbm] * 5,
        out_specs=(vmem, vmem, vmem),
        scratch_shapes=[
            pltpu.SMEM(pair_local.shape, jnp.int32),
            pltpu.SMEM(pair_other.shape, jnp.int32),
            pltpu.VMEM(positions.shape, f32),
            pltpu.VMEM(positions.shape, f32),
            pltpu.VMEM((tile_dev, LANES), f32),
            pltpu.VMEM((bead_count, sub), f32),
            pltpu.VMEM(matrices.shape, f32),
            dma((7,)),
            pltpu.VMEM((2,) + positions.shape, f32),
            pltpu.VMEM((2, tile_dev, LANES), f32),
            pltpu.VMEM((tile_dev, deep, rows * LANES), jnp.bfloat16),
            pltpu.VMEM((3 * tile_dev, LANES, deep), jnp.bfloat16),
            pltpu.VMEM((3 * tile_dev, LANES, 8), f32),
            pltpu.VMEM((tile_dev, rows, LANES), f32),
            pltpu.VMEM((rows, atom_dev), f32),
            pltpu.VMEM((bead_count, rows, sub), f32),
            pltpu.VMEM((bead_count, rows, sub), f32),
            pltpu.VMEM((bead_count, rows, sub), f32),
            pltpu.VMEM((bead_count, rows, sub), f32),
            pltpu.VMEM((bead_count, 2 * rows + 1, sub), f32),
            pltpu.VMEM((bead_count, 2 * rows + 1, sub), f32),
            pltpu.VMEM((3 * beads, sub), f32),
            pltpu.VMEM((3 * beads, sub), f32),
            dma((2, 2)),
            dma((2, 2)),
        ]
        + [dma((bead_count,))] * 6,
        compiler_params=pltpu.CompilerParams(collective_id=0, has_side_effects=True),
    )(
        pair_local, pair_other, pair_count, positions, momenta,
        charge.reshape(tile_dev, LANES), masses.reshape(bead_count, sub),
        jnp.asarray(matrices),
    )
    results = (new_positions, new_momenta, spring)
    new_positions, new_momenta, spring = pl.pallas_call(
        hand_over,
        out_shape=tuple(jax.ShapeDtypeStruct(v.shape, f32) for v in results),
        in_specs=[vmem] * 3,
        out_specs=(vmem,) * 3,
    )(*results)
    back = (1, 0, 2)
    return (
        jnp.transpose(new_positions, back),
        jnp.transpose(new_momenta, back),
        spring.reshape(atom_dev),
    )


def solution(mesh):
    return jax.shard_map(
        on_device,
        mesh=mesh,
        in_specs=(
            P("bead", None, "atom"),
            P("bead", None, "atom"),
            P("atom"),
            P("atom"),
            P("atom"),
            P("atom"),
            P("atom"),
        ),
        out_specs=(P("bead", None, "atom"), P("bead", None, "atom"), P("atom")),
        check_vma=False,
    )
```
